32 devices in a mesh: section: 8 (over y, x, core), tensor: 4 (over z).
Axes of the slice: x: 2, y: 2, z: 4, core: 2. Of those that a mesh axis runs over, the one named last changes fastest.
Arguments:
- arriving: bfloat16 [8, 512, 16384], P('section', 'tensor'), may hold values from -6 to 6
- kept_input: bfloat16 [8, 512, 16384], P('section', 'tensor'), may hold values from -6 to 6
- returning: bfloat16 [8, 512, 16384], P('section', 'tensor'), may hold values from -6 to 6
- norm_gain: bfloat16 [8, 16384], P('section'), may hold values from 0.25 to 1.75
- key_weight: bfloat16 [8, 16384, 1024], P('section', 'tensor'), may hold values from -0.0625 to 0.0625
- value_weight: bfloat16 [8, 16384, 1024], P('section', 'tensor'), may hold values from -0.0625 to 0.0625
- key_down: bfloat16 [8, 16384, 16], P('section', 'tensor'), may hold values from -0.046875 to 0.046875
- value_down: bfloat16 [8, 16384, 16], P('section', 'tensor'), may hold values from -0.046875 to 0.046875
- key_up: bfloat16 [8, 16, 1024], P('section', None, 'tensor'), may hold values from -1.5 to 1.5
- value_up: bfloat16 [8, 16, 1024], P('section', None, 'tensor'), may hold values from -1.5 to 1.5
- key_cot: bfloat16 [8, 512, 1024], P('section', None, 'tensor'), may hold values from -6 to 6
- value_cot: bfloat16 [8, 512, 1024], P('section', None, 'tensor'), may hold values from -6 to 6
Outputs:
- keys: bfloat16 [8, 512, 1024], P('section', None, 'tensor')
- values: bfloat16 [8, 512, 1024], P('section', None, 'tensor')
- input_grad: bfloat16 [8, 512, 16384], P('section', 'tensor')
- key_down_grad: float32 [8, 16384, 16], P('section', 'tensor')
- value_down_grad: float32 [8, 16384, 16], P('section', 'tensor')
- key_up_grad: float32 [8, 16, 1024], P('section', None, 'tensor')
- value_up_grad: float32 [8, 16, 1024], P('section', None, 'tensor')
The draws below stay inside these ranges and needn't reach their ends.
All inputs are finite; a program needn't handle non-finite values.
Results may differ from the reference program's by a relative error of at most 0.014.
Values may be sent and summed in bfloat16 or wider, within the bound.
No kernel may reach another device: no remote copies, remote signals or barrier semaphores. Data moves between devices by JAX's collectives and lax.ppermute only.
A program may use at most 192 MiB of HBM per device.

```python
import jax
import jax.numpy as jnp
from jax import lax

D = 16384
RANK = 16
TOKENS = 512
KVW = 1024
LAYERS = 8


def with_spikes(values, stream_key, source, target, blocks, factor):
    def block_of(position):
        return (jnp.arange(values.shape[position]) // (values.shape[position] // blocks)).reshape((-1,) + (1,) * (values.ndim - 1 - position))

    one_side = jax.random.permutation(stream_key, blocks)[block_of(target)]
    other_side = (block_of(target) + blocks // 2) % blocks
    return jnp.where((block_of(source) == one_side) | (block_of(source) == other_side), factor * values, values)


def block_scale(stream_key, dims, cuts, low, high):
    level = 1.0
    for position, shards_of in cuts:
        draws = jax.random.uniform(jax.random.fold_in(jax.random.fold_in(stream_key, 6), position), (shards_of,), jnp.float32, low / len(cuts), high / len(cuts))
        level = level * jnp.repeat(jnp.exp(draws), dims[position] // shards_of).reshape((-1,) + (1,) * (len(dims) - 1 - position))
    return level


def bell_draw(key, extent, scale, reach, shards=(), held_as=jnp.bfloat16):
    factor_of = block_scale(key, extent, shards, -0.22, 0.18) if shards else 1.0
    result = jax.random.normal(key, extent, jnp.float32) * scale * factor_of
    return jnp.minimum(jnp.maximum(result, -reach), reach).astype(held_as)


def noise_with(stream_key, extent, spread, bound, pieces, heavy, dtype=jnp.bfloat16):
    entries = spread * jax.random.normal(stream_key, extent, jnp.float32)
    if pieces:
        entries = entries * block_scale(stream_key, extent, pieces, -0.22, 0.18)
    return jnp.clip(with_spikes(entries, jax.random.fold_in(stream_key, 3), *heavy), -bound, bound).astype(dtype)


def setup_inputs(seed: int = 0) -> dict:
    key_of = jax.random.split(jax.random.key(seed), 13)
    return {
        "arriving": bell_draw(key_of[0], (LAYERS, TOKENS, D), 1.0, 6.0, ((0, 8), (1, 4))),
        "kept_input": bell_draw(key_of[1], (LAYERS, TOKENS, D), 1.0, 6.0, ((0, 8), (1, 4))),
        "returning": bell_draw(key_of[2], (LAYERS, TOKENS, D), 1.0, 6.0, ((0, 8), (1, 4))),
        "norm_gain": jnp.clip(1.0 + 0.15 * jax.random.normal(key_of[3], (LAYERS, D), jnp.float32), 0.25, 1.75).astype(jnp.bfloat16),
        "key_weight": noise_with(key_of[4], (LAYERS, D, KVW), D ** -0.5, 0.0625, ((0, 8), (1, 4)), (1, 2, 4, 2.0)),
        "value_weight": noise_with(key_of[5], (LAYERS, D, KVW), D ** -0.5, 0.0625, ((0, 8), (1, 4)), (1, 2, 4, 2.0)),
        "key_down": bell_draw(key_of[6], (LAYERS, D, RANK), D ** -0.5, 0.046875, ((0, 8), (1, 4))),
        "value_down": bell_draw(key_of[7], (LAYERS, D, RANK), D ** -0.5, 0.046875, ((0, 8), (1, 4))),
        "key_up": bell_draw(key_of[8], (LAYERS, RANK, KVW), RANK ** -0.5, 1.5, ((0, 8), (2, 4))),
        "value_up": bell_draw(key_of[9], (LAYERS, RANK, KVW), RANK ** -0.5, 1.5, ((0, 8), (2, 4))),
        "key_cot": bell_draw(key_of[10], (LAYERS, TOKENS, KVW), 1.0, 6.0, ((0, 8), (2, 4))),
        "value_cot": bell_draw(key_of[11], (LAYERS, TOKENS, KVW), 1.0, 6.0, ((0, 8), (2, 4))),
    }


epsilon = 1e-05
adapter_scale = 2.0

def normalize(hidden, gain):
    values = hidden.astype(jnp.float32)
    inverse = lax.rsqrt(lax.optimization_barrier(jnp.mean(values * values, axis=-1, keepdims=True)) + epsilon)
    return (inverse, (values * inverse * gain.astype(jnp.float32)).astype(jnp.bfloat16))

def precise_product(left, right):
    return jnp.dot(left, right, precision=lax.Precision.HIGHEST, preferred_element_type=jnp.float32)

def mixed_product(left, right):
    return jnp.dot(left.astype(jnp.float32), right.astype(jnp.float32), preferred_element_type=jnp.float32)

def one_layer(blocks):
    incoming, kept, back, gain, key_matrix, value_matrix, key_down_matrix, value_down_matrix, key_up_matrix, value_up_matrix, key_cotangent, value_cotangent = blocks
    _, normed_input = normalize(incoming, gain)
    key_middle = mixed_product(normed_input, key_down_matrix)
    value_middle = mixed_product(normed_input, value_down_matrix)
    keys = (mixed_product(normed_input, key_matrix) + adapter_scale * precise_product(key_middle, key_up_matrix.astype(jnp.float32))).astype(jnp.bfloat16)
    values = (mixed_product(normed_input, value_matrix) + adapter_scale * precise_product(value_middle, value_up_matrix.astype(jnp.float32))).astype(jnp.bfloat16)
    adapted_key = mixed_product(key_cotangent, key_up_matrix.T)
    adapted_value = mixed_product(value_cotangent, value_up_matrix.T)
    branch_output = mixed_product(key_cotangent, key_matrix.T) + mixed_product(value_cotangent, value_matrix.T)
    branch_output = branch_output + adapter_scale * (precise_product(adapted_key, key_down_matrix.T.astype(jnp.float32)) + precise_product(adapted_value, value_down_matrix.T.astype(jnp.float32)))
    branch_output = lax.optimization_barrier(branch_output.astype(jnp.bfloat16)).astype(jnp.float32)
    inverse, kept_normed = normalize(kept, gain)
    kept_values = kept.astype(jnp.float32)
    scaled = gain.astype(jnp.float32) * branch_output
    inner = lax.optimization_barrier(jnp.mean(kept_values * scaled, axis=-1, keepdims=True))
    input_grad = (back.astype(jnp.float32) + inverse * scaled - kept_values * inverse * inverse * inverse * inner).astype(jnp.bfloat16)
    saved_wide_input = kept_normed.astype(jnp.float32)
    key_down_gradient = adapter_scale * precise_product(saved_wide_input.T, adapted_key)
    value_down_gradient = adapter_scale * precise_product(saved_wide_input.T, adapted_value)
    key_middle_rows = mixed_product(kept_normed, key_down_matrix)
    value_middle_rows = mixed_product(kept_normed, value_down_matrix)
    key_up_gradient = adapter_scale * precise_product(key_middle_rows.T, key_cotangent.astype(jnp.float32))
    value_up_gradient = adapter_scale * precise_product(value_middle_rows.T, value_cotangent.astype(jnp.float32))
    return (keys, values, input_grad, key_down_gradient, value_down_gradient, key_up_gradient, value_up_gradient)

def reference(arriving, kept_input, returning, norm_gain, key_weight, value_weight, key_down, value_down, key_up, value_up, key_cot, value_cot):
    incoming = jnp.roll(arriving, 1, axis=0)
    back = jnp.roll(returning, -1, axis=0)
    layer_count = arriving.shape[0]
    collected = []
    for layer in range(layer_count):
        blocks = (incoming[layer], kept_input[layer], back[layer], norm_gain[layer], key_weight[layer], value_weight[layer], key_down[layer], value_down[layer], key_up[layer], value_up[layer], key_cot[layer], value_cot[layer])
        collected.append(one_layer(blocks))
    stacked = [jnp.stack([item[index] for item in collected], axis=0) for index in range(7)]
    return (stacked[0], stacked[1], stacked[2], stacked[3], stacked[4], stacked[5], stacked[6])
```

```python
import jax
import jax.numpy as jnp
from jax import lax
from jax.sharding import PartitionSpec as P

epsilon = 1e-05
adapter_scale = 2.0
bf16 = jnp.bfloat16
f32 = jnp.float32


def send(x, section_by, tensor_by):
    sections = lax.axis_size("section")
    tensors = lax.axis_size("tensor")
    pairs = [
        (s * tensors + t, ((s + section_by) % sections) * tensors + (t + tensor_by) % tensors)
        for s in range(sections)
        for t in range(tensors)
    ]
    return lax.ppermute(x, ("section", "tensor"), pairs)


def move(x, section_by, tensor_by):
    if section_by == 0 and tensor_by == 0:
        return x
    return send(x, section_by, tensor_by)


def dot(left, right, left_dim, right_dim, precision=None):
    return lax.dot_general(
        left,
        right,
        (((left_dim,), (right_dim,)), ((), ())),
        precision=precision,
        preferred_element_type=f32,
    )


def inverse_of(hidden):
    values = hidden.astype(f32)
    return lax.rsqrt(jnp.mean(values * values, axis=-1) + epsilon)


def on_device(
    arriving,
    kept_input,
    returning,
    norm_gain,
    key_weight,
    value_weight,
    key_down,
    value_down,
    key_up,
    value_up,
    key_cot,
    value_cot,
):
    count = lax.axis_size("tensor")
    me = lax.axis_index("tensor")
    to = [(me + k) % count for k in range(count)]
    source = [(me - k) % count for k in range(count)]
    gain = norm_gain[0]
    sent = arriving[0]
    kept = kept_input[0]
    rows, width = sent.shape
    feats = width // count
    tokens = rows * count
    rank = key_up.shape[1]
    heads = key_up.shape[2]
    down = jnp.concatenate([key_down[0].T, value_down[0].T], axis=0)

    packed = jnp.concatenate(
        [
            jnp.concatenate([key_cot[0], value_cot[0]], axis=1),
            jnp.concatenate([key_up[0], value_up[0]], axis=1),
        ],
        axis=0,
    )
    packed_all = lax.all_gather(packed, "tensor", axis=0)
    down_all = lax.all_gather(down, "tensor", axis=0)

    sent_inverse = inverse_of(sent).reshape(1, rows)
    arrived = []
    arrived_inverse = []
    for k in range(count):
        piece = lax.dynamic_slice_in_dim(sent, to[k] * feats, feats, 1)
        arrived.append(send(piece, 1, k))
        arrived_inverse.append(send(sent_inverse, 1, k))
    back = send(returning[0], -1, 0)

    cots_all = jnp.transpose(packed_all, (1, 0, 2))
    key_all = cots_all[:, :, :heads].reshape(tokens + rank, count * heads)
    value_all = cots_all[:, :, heads:].reshape(tokens + rank, count * heads)
    key_cot_all, key_up_all = key_all[:tokens], key_all[tokens:]
    value_cot_all, value_up_all = value_all[:tokens], value_all[tokens:]
    adapted = jnp.concatenate(
        [dot(key_cot_all, key_up_all, 1, 1), dot(value_cot_all, value_up_all, 1, 1)], axis=1
    )
    adapted16 = (adapter_scale * adapted).astype(bf16)
    branch = (
        dot(key_cot_all, key_weight[0], 1, 1)
        + dot(value_cot_all, value_weight[0], 1, 1)
        + dot(adapted16, down, 1, 0)
    ).astype(bf16)
    branch_rows = jnp.zeros((rows, width), bf16)
    for k in range(count):
        piece = lax.dynamic_slice_in_dim(branch, to[k] * rows, rows, 0)
        got = move(piece, 0, k)
        branch_rows = lax.dynamic_update_slice_in_dim(branch_rows, got, source[k] * feats, 1)

    kept_inverse = inverse_of(kept)[:, None]
    kept_normed = (kept.astype(f32) * kept_inverse * gain.astype(f32)).astype(bf16)
    mine = lax.dynamic_slice_in_dim(adapted16, me * rows, rows, 0)
    down_partial = dot(mine, kept_normed, 0, 0).astype(bf16)
    down_gradient = jnp.zeros((2 * rank, feats), f32)
    for k in range(count):
        piece = lax.dynamic_slice_in_dim(down_partial, to[k] * feats, feats, 1)
        down_gradient = down_gradient + move(piece, 0, k).astype(f32)
    down_whole = jnp.transpose(down_all, (1, 0, 2)).reshape(2 * rank, width)
    middle = dot(down_whole, kept_normed, 1, 1)
    middles = jnp.zeros((2 * rank, tokens), f32)
    for k in range(count):
        middles = lax.dynamic_update_slice_in_dim(
            middles, move(middle, 0, k), source[k] * rows, 1
        )
    exact = lax.Precision.HIGHEST
    key_up_gradient = adapter_scale * dot(middles[:rank], key_cot[0].astype(f32), 1, 0, exact)
    value_up_gradient = adapter_scale * dot(middles[rank:], value_cot[0].astype(f32), 1, 0, exact)

    my_gain = lax.dynamic_slice_in_dim(gain, me * feats, feats, 0).astype(f32)
    spread = jnp.zeros((tokens, feats), bf16)
    for k in range(count):
        normed = (
            arrived[k].astype(f32) * arrived_inverse[k].reshape(rows, 1) * my_gain
        ).astype(bf16)
        spread = lax.dynamic_update_slice_in_dim(spread, normed, source[k] * rows, 0)
    mids = (adapter_scale * dot(spread, down, 1, 1)).astype(bf16)
    key_partial = dot(spread, key_weight[0], 1, 0) + dot(mids[:, :rank], key_up_all, 1, 0)
    value_partial = dot(spread, value_weight[0], 1, 0) + dot(mids[:, rank:], value_up_all, 1, 0)
    key_partial = key_partial.astype(bf16)
    value_partial = value_partial.astype(bf16)
    key_sum = 0.0
    value_sum = 0.0
    for k in range(count):
        piece = jnp.concatenate(
            [
                lax.dynamic_slice_in_dim(key_partial, to[k] * heads, heads, 1),
                lax.dynamic_slice_in_dim(value_partial, to[k] * heads, heads, 1),
            ],
            axis=1,
        )
        got = move(piece, 0, k).astype(f32)
        key_sum = key_sum + got[:, :heads]
        value_sum = value_sum + got[:, heads:]
    keys = key_sum.astype(bf16)
    values = value_sum.astype(bf16)

    kept_values = kept.astype(f32)
    scaled = gain.astype(f32) * branch_rows.astype(f32)
    inner = jnp.mean(kept_values * scaled, axis=-1, keepdims=True)
    input_grad = (
        back.astype(f32)
        + kept_inverse * scaled
        - kept_values * (kept_inverse * kept_inverse * kept_inverse * inner)
    ).astype(bf16)
    return (
        keys[None],
        values[None],
        input_grad[None],
        down_gradient[:rank].T[None],
        down_gradient[rank:].T[None],
        key_up_gradient[None],
        value_up_gradient[None],
    )


def solution(mesh):
    return jax.shard_map(
        on_device,
        mesh=mesh,
        in_specs=(
            P("section", "tensor", None),
            P("section", "tensor", None),
            P("section", "tensor", None),
            P("section", None),
            P("section", "tensor", None),
            P("section", "tensor", None),
            P("section", "tensor", None),
            P("section", "tensor", None),
            P("section", None, "tensor"),
            P("section", None, "tensor"),
            P("section", None, "tensor"),
            P("section", None, "tensor"),
        ),
        out_specs=(
            P("section", None, "tensor"),
            P("section", None, "tensor"),
            P("section", "tensor", None),
            P("section", "tensor", None),
            P("section", "tensor", None),
            P("section", None, "tensor"),
            P("section", None, "tensor"),
        ),
        check_vma=False,
    )
```

```python
import jax
import jax.numpy as jnp
from jax import lax
from jax.sharding import PartitionSpec as P


epsilon = 1e-05
adapter_scale = 2.0
bf16 = jnp.bfloat16
f32 = jnp.float32


def send(x, section_by, tensor_by):
    sections = lax.axis_size("section")
    tensors = lax.axis_size("tensor")
    pairs = [
        (s * tensors + t, ((s + section_by) % sections) * tensors + (t + tensor_by) % tensors)
        for s in range(sections)
        for t in range(tensors)
    ]
    return lax.ppermute(x, ("section", "tensor"), pairs)


def move(x, section_by, tensor_by):
    if section_by == 0 and tensor_by == 0:
        return x
    return send(x, section_by, tensor_by)


def exchange(x, bit):
    sections = lax.axis_size("section")
    tensors = lax.axis_size("tensor")
    pairs = [
        (s * tensors + t, s * tensors + (t ^ bit)) for s in range(sections) for t in range(tensors)
    ]
    return lax.ppermute(x, ("section", "tensor"), pairs)


def halving_sum(blocks):
    count = lax.axis_size("tensor")
    assert count & (count - 1) == 0
    me = lax.axis_index("tensor")
    bit = 1
    while bit < count:
        pairs = blocks.reshape((blocks.shape[0] // 2, 2) + blocks.shape[1:])
        side = (me // bit) % 2
        kept = lax.dynamic_index_in_dim(pairs, side, 1, keepdims=False)
        given = lax.dynamic_index_in_dim(pairs, 1 - side, 1, keepdims=False)
        given = given.astype(bf16)
        got = exchange(given, bit)
        blocks = kept.astype(f32) + got.astype(f32)
        bit *= 2
    return blocks[0]


def dot(left, right, left_dim, right_dim, precision=None):
    return lax.dot_general(
        left,
        right,
        (((left_dim,), (right_dim,)), ((), ())),
        precision=precision,
        preferred_element_type=f32,
    )


def inverse_of(hidden):
    values = hidden.astype(f32)
    return lax.rsqrt(jnp.mean(values * values, axis=-1) + epsilon)


def on_device(
    arriving,
    kept_input,
    returning,
    norm_gain,
    key_weight,
    value_weight,
    key_down,
    value_down,
    key_up,
    value_up,
    key_cot,
    value_cot,
):
    count = lax.axis_size("tensor")
    me = lax.axis_index("tensor")
    to = [(me + k) % count for k in range(count)]
    source = [(me - k) % count for k in range(count)]
    gain = norm_gain[0]
    sent = arriving[0]
    kept = kept_input[0]
    rows, width = sent.shape
    feats = width // count
    tokens = rows * count
    rank = key_up.shape[1]
    heads = key_up.shape[2]
    down = jnp.concatenate([key_down[0].T, value_down[0].T], axis=0)

    packed = jnp.concatenate(
        [
            jnp.concatenate([key_cot[0], value_cot[0]], axis=1),
            jnp.concatenate([key_up[0], value_up[0]], axis=1),
        ],
        axis=0,
    )
    packed_all = lax.all_gather(packed, "tensor", axis=0)
    down_all = lax.all_gather(down, "tensor", axis=0)

    sent_inverse = inverse_of(sent).reshape(1, rows)
    pieces = [lax.dynamic_slice_in_dim(sent, to[k] * feats, feats, 1) for k in range(count)]
    packed_all, pieces[2:] = lax.optimization_barrier((packed_all, pieces[2:]))
    arrived = []
    for k in range(count):
        arrived.append(send(pieces[k], 1, k))
    arrived_inverse = [send(sent_inverse, 1, k) for k in range(count)]
    back = send(returning[0], -1, 0)

    cots_all = jnp.transpose(packed_all, (1, 0, 2))
    key_all = cots_all[:, :, :heads].reshape(tokens + rank, count * heads)
    value_all = cots_all[:, :, heads:].reshape(tokens + rank, count * heads)
    key_cot_all, key_up_all = key_all[:tokens], key_all[tokens:]
    value_cot_all, value_up_all = value_all[:tokens], value_all[tokens:]
    adapted = jnp.concatenate(
        [dot(key_cot_all, key_up_all, 1, 1), dot(value_cot_all, value_up_all, 1, 1)], axis=1
    )
    adapted16 = (adapter_scale * adapted).astype(bf16)
    branch = (
        dot(key_cot_all, key_weight[0], 1, 1)
        + dot(value_cot_all, value_weight[0], 1, 1)
        + dot(adapted16, down, 1, 0)
    ).astype(bf16)
    kept_inverse = inverse_of(kept)[:, None]
    kept_normed = (kept.astype(f32) * kept_inverse * gain.astype(f32)).astype(bf16)
    mine = lax.dynamic_slice_in_dim(adapted16, me * rows, rows, 0)
    down_partial = dot(mine, kept_normed, 0, 0)
    branch_rows = jnp.zeros((rows, width), bf16)
    for k in range(count):
        piece = lax.dynamic_slice_in_dim(branch, to[k] * rows, rows, 0)
        got = move(piece, 0, k)
        branch_rows = lax.dynamic_update_slice_in_dim(branch_rows, got, source[k] * feats, 1)

    down_blocks = jnp.transpose(down_partial.reshape(2 * rank, count, feats), (1, 0, 2))
    down_gradient = halving_sum(down_blocks)
    down_whole = jnp.transpose(down_all, (1, 0, 2)).reshape(2 * rank, width)
    middle = dot(down_whole, kept_normed, 1, 1)
    middles = jnp.zeros((2 * rank, tokens), f32)
    for k in range(count):
        got = move(middle, 0, k)
        middles = lax.dynamic_update_slice_in_dim(middles, got, source[k] * rows, 1)

    my_gain = lax.dynamic_slice_in_dim(gain, me * feats, feats, 0).astype(f32)
    spread = jnp.zeros((tokens, feats), bf16)
    for k in range(count):
        normed = (
            arrived[k].astype(f32) * arrived_inverse[k].reshape(rows, 1) * my_gain
        ).astype(bf16)
        spread = lax.dynamic_update_slice_in_dim(spread, normed, source[k] * rows, 0)
    spread, middles = lax.optimization_barrier((spread, middles))
    mids = (adapter_scale * dot(spread, down, 1, 1)).astype(bf16)
    key_partial = dot(spread, key_weight[0], 1, 0) + dot(mids[:, :rank], key_up_all, 1, 0)
    value_partial = dot(spread, value_weight[0], 1, 0) + dot(mids[:, rank:], value_up_all, 1, 0)
    partial = jnp.stack([key_partial, value_partial]).reshape(2, tokens, count, heads)
    sums = halving_sum(jnp.transpose(partial, (2, 0, 1, 3)))
    keys = sums[0].astype(bf16)
    values = sums[1].astype(bf16)

    exact = lax.Precision.HIGHEST
    key_up_gradient = adapter_scale * dot(middles[:rank], key_cot[0].astype(f32), 1, 0, exact)
    value_up_gradient = adapter_scale * dot(middles[rank:], value_cot[0].astype(f32), 1, 0, exact)
    branch_rows, key_up_gradient, value_up_gradient, down_gradient = lax.optimization_barrier(
        (branch_rows, key_up_gradient, value_up_gradient, down_gradient)
    )

    kept_values = kept.astype(f32)
    scaled = gain.astype(f32) * branch_rows.astype(f32)
    inner = jnp.mean(kept_values * scaled, axis=-1, keepdims=True)
    input_grad = (
        back.astype(f32)
        + kept_inverse * scaled
        - kept_values * (kept_inverse * kept_inverse * kept_inverse * inner)
    ).astype(bf16)
    return (
        keys[None],
        values[None],
        input_grad[None],
        down_gradient[:rank].T[None],
        down_gradient[rank:].T[None],
        key_up_gradient[None],
        value_up_gradient[None],
    )


def solution(mesh):
    return jax.shard_map(
        on_device,
        mesh=mesh,
        in_specs=(
            P("section", "tensor", None),
            P("section", "tensor", None),
            P("section", "tensor", None),
            P("section", None),
            P("section", "tensor", None),
            P("section", "tensor", None),
            P("section", "tensor", None),
            P("section", "tensor", None),
            P("section", None, "tensor"),
            P("section", None, "tensor"),
            P("section", None, "tensor"),
            P("section", None, "tensor"),
        ),
        out_specs=(
            P("section", None, "tensor"),
            P("section", None, "tensor"),
            P("section", "tensor", None),
            P("section", "tensor", None),
            P("section", "tensor", None),
            P("section", None, "tensor"),
            P("section", None, "tensor"),
        ),
        check_vma=False,
    )
```
